512 devices in a mesh: grp: 2 (over y), tx: 16 (over z), ty: 16 (over x, core).
Axes of the slice: x: 8, y: 2, z: 16, core: 2. Of those that a mesh axis runs over, the one named last changes fastest.
The devices are a block of a 8x8x16 slice.
Arguments:
- obj_field: float32 [2, 4096, 2048], P(None, ('grp', 'tx'), 'ty'), parts along dimension 1, may hold values from -6 to 6
- eigenprobes: bfloat16 [2, 32, 128, 128], P(None, 'grp'), parts along dimension 1, may hold values from -1.5 to 1.5
- weights: float32 [32, 16, 3, 16], P(('grp', 'tx'), 'ty'), parts along dimension 0, may hold values from -4 to 4
- offsets: int32 [32, 16, 3, 2], P(('grp', 'tx'), 'ty'), parts along dimension 0, may hold values from 0 to 127
- counts: int32 [32, 16], P(('grp', 'tx'), 'ty'), parts along dimension 0, may hold values from 1 to 3, as said below
- amplitudes: bfloat16 [32, 16, 3, 128, 128], P(('grp', 'tx'), 'ty'), parts along dimension 0, may hold values from 0.19921875 to 3
Outputs:
- new_object: float32 [2, 4096, 2048], P(None, ('grp', 'tx'), 'ty'), parts along dimension 1
- new_eigenprobes: float32 [2, 32, 128, 128], P(None, 'grp'), parts along dimension 1
The draws below stay inside these ranges and needn't reach their ends.
There are 2 independent parts, one for each index of `grp`. The reference program is written for one: setup_inputs(seed, part) draws one part's arguments, and reference() takes and returns one part's arrays. A program takes and returns all parts, laid end to end along the dimension named above; each array names one. Nothing has to cross between parts.
Inputs may be any that keep to these rules, and one draw needn't show every extreme that they name: Every tile holds 1 to 3 positions; some tile holds exactly 3; slots from counts on are unused.
All inputs are finite; a program needn't handle non-finite values.
Results may differ from the reference program's by a relative error of at most 0.0003.
Values sent between devices are 32-bit elements; how exact they have to be, the bound alone decides.
No kernel may reach another device: no remote copies, remote signals or barrier semaphores. Data moves between devices by JAX's collectives and lax.ppermute only.
A program may use at most 64 MiB of HBM per device.

```python
import math
import jax
import jax.numpy as jnp
from jax import lax

FRAME = 128
MODES = 16
TILE = 128
SLOTS = 3
HEIGHT = 2048
WIDTH = 2048
N_TX = 16
N_TY = 16


def draw_counts(key, part):
    first_key = jax.random.fold_in(key, 11)
    second_key = jax.random.fold_in(key, 12)
    spot_key = jax.random.fold_in(key, 13)
    first = jax.random.randint(first_key, (N_TX * N_TY,), 0, SLOTS)
    second = jax.random.randint(second_key, (N_TX * N_TY,), 0, SLOTS)
    loads = 1 + first * second // SLOTS
    spot = jax.random.randint(spot_key, (), 0, N_TX * N_TY)
    loads = jnp.where(jnp.arange(N_TX * N_TY) == spot, SLOTS, loads)
    return loads.reshape(N_TX, N_TY).astype(jnp.int32)


def plant(drawn, stream_key, smallest, largest):
    extent = drawn.shape
    place = [jax.random.randint(jax.random.fold_in(stream_key, axis), (), 0, extent[axis]) for axis in range(len(extent))]
    drawn = drawn.at[tuple(place)].set(smallest)
    longest = extent.index(max(extent))
    place[longest] = (place[longest] + 1) % extent[longest]
    return drawn.at[tuple(place)].set(largest)


def block_levels(stream_key, shape, shards, least, high):
    factor_of = 1.0
    for position, shards_of in shards:
        heights = jax.random.uniform(jax.random.fold_in(jax.random.fold_in(stream_key, 6), position), (shards_of,), jnp.float32, least / len(shards), high / len(shards))
        factor_of = factor_of * jnp.repeat(jnp.exp(heights), shape[position] // shards_of).reshape((-1,) + (1,) * (len(shape) - 1 - position))
    return factor_of


def scatter_about(stream_key, dims, scale, reach, split=(), kind=jnp.bfloat16):
    level = block_levels(stream_key, dims, split, -0.22, 0.18) if split else 1.0
    drawn = jax.random.normal(stream_key, dims, jnp.float32) * scale * level
    return jnp.minimum(jnp.maximum(drawn, -reach), reach).astype(kind)


def setup_inputs(seed: int = 0, part: int = 0) -> dict:
    arg_keys = jax.random.split(jax.random.key(seed), 7)
    own_keys = jax.random.split(jax.random.fold_in(arg_keys[6], part), 7)
    obj_field = scatter_about(own_keys[0], (2, HEIGHT, WIDTH), 1.0, 6.0, ((1, 16), (2, 16)), jnp.float32)
    eigenprobes = scatter_about(own_keys[1], (2, MODES, FRAME, FRAME), 0.25, 1.5)
    weights = scatter_about(own_keys[2], (N_TX, N_TY, SLOTS, MODES), 1.0, 4.0, ((0, 16), (1, 16)), jnp.float32)
    offsets = plant(jax.random.randint(own_keys[3], (N_TX, N_TY, SLOTS, 2), 0, TILE), jax.random.fold_in(own_keys[3], 1), 0, TILE - 1).astype(jnp.int32)
    counts = draw_counts(jax.random.fold_in(jax.random.fold_in(arg_keys[6], part), 71), part)
    amplitudes = jnp.clip(jnp.exp(math.log(3.0) - 2.7119641 * jax.random.uniform(own_keys[5], (N_TX, N_TY, SLOTS, FRAME, FRAME), jnp.float32) ** block_levels(own_keys[5], (N_TX, N_TY, SLOTS, FRAME, FRAME), ((0, 16), (1, 16)), -0.2, 0.2)), 0.19921875, 3.0).astype(jnp.bfloat16)
    return {"obj_field": obj_field, "eigenprobes": eigenprobes, "weights": weights, "offsets": offsets, "counts": counts, "amplitudes": amplitudes}


def reference(obj_field, eigenprobes, weights, offsets, counts, amplitudes):
    height = obj_field.shape[1]
    width = obj_field.shape[2]
    eig = eigenprobes.astype(jnp.float32)
    ocomplex = lax.complex(obj_field[0], obj_field[1])
    ecomplex = lax.complex(eig[0], eig[1])
    idx = jnp.arange(FRAME, dtype=jnp.int32)
    slot_ids = jnp.arange(SLOTS, dtype=jnp.int32)
    high = lax.Precision.HIGHEST

    def one_tile(carry, flat):
        gobj, illum, gprobe, norms = carry
        row_tile = flat // N_TY
        col_tile = flat % N_TY
        wts = weights[row_tile, col_tile]
        offs = offsets[row_tile, col_tile]
        live = (slot_ids < counts[row_tile, col_tile]).astype(obj_field.dtype)
        amps = amplitudes[row_tile, col_tile].astype(obj_field.dtype)
        rows = ((row_tile * TILE + offs[:, 0])[:, None] + idx[None, :]).astype(jnp.int32) % height
        cols = ((col_tile * TILE + offs[:, 1])[:, None] + idx[None, :]).astype(jnp.int32) % width
        win = ocomplex[rows[:, :, None], cols[:, None, :]]
        probe_re = jnp.einsum('sk,kij->sij', wts, eig[0], precision=high)
        probe_im = jnp.einsum('sk,kij->sij', wts, eig[1], precision=high)
        probe = lax.complex(probe_re, probe_im)
        spec = jnp.fft.fft2(probe * win, norm='ortho')
        mag = jnp.sqrt(jnp.real(spec) ** 2 + jnp.imag(spec) ** 2 + 0.25)
        factor = (amps / mag - 1.0) * live[:, None, None]
        chi = jnp.fft.ifft2(spec * factor, norm='ortho')
        gobj = gobj.at[rows[:, :, None], cols[:, None, :]].add(jnp.conj(probe) * chi)
        power = (probe_re ** 2 + probe_im ** 2) * live[:, None, None]
        illum = illum.at[rows[:, :, None], cols[:, None, :]].add(power)
        grad = jnp.conj(win) * chi
        add_re = jnp.einsum('sk,sij->kij', wts, jnp.real(grad), precision=high)
        add_im = jnp.einsum('sk,sij->kij', wts, jnp.imag(grad), precision=high)
        gprobe = gprobe + lax.complex(add_re, add_im)
        norms = norms + lax.optimization_barrier(jnp.sum(live[:, None] * wts * wts, axis=0))
        return ((gobj, illum, gprobe, norms), None)
    start = (jnp.zeros_like(ocomplex), jnp.zeros_like(obj_field[0]), jnp.zeros_like(ecomplex), jnp.zeros((MODES,), obj_field.dtype))
    (gobj, illum, gprobe, norms), _ = lax.scan(one_tile, start, jnp.arange(N_TX * N_TY, dtype=jnp.int32))
    mean_illum = jnp.sum(illum) / (height * width)
    new_obj = ocomplex + gobj / (illum + mean_illum)
    new_eig = ecomplex + gprobe / (norms + 1.0)[:, None, None]
    return (jnp.stack([jnp.real(new_obj), jnp.imag(new_obj)]), jnp.stack([jnp.real(new_eig), jnp.imag(new_eig)]))
```

```python
import math

import jax
import jax.numpy as jnp
from jax import lax
from jax.sharding import Mesh
from jax.sharding import PartitionSpec as P

TY = ("ty_0", "ty_1")
PART = ("tx", "ty_0", "ty_1")

high = lax.Precision.HIGHEST


def moved(value, down, right):
    rows = lax.axis_size("tx")
    cols = lax.axis_size("ty_0") * lax.axis_size("ty_1")
    pairs = [
        (i * cols + j, ((i + down) % rows) * cols + (j + right) % cols)
        for i in range(rows)
        for j in range(cols)
    ]
    return lax.ppermute(value, PART, pairs)


def exchanged(blocks, axis):
    return lax.all_to_all(blocks, axis, split_axis=0, concat_axis=0, tiled=True)


def copied_to_all(block, axis):
    count = lax.axis_size(axis)
    return exchanged(jnp.broadcast_to(block[None], (count, *block.shape)), axis)


def tables(frame, sign):
    grid = jnp.arange(frame, dtype=jnp.int32)
    phase = grid[:, None] * grid[None, :] % frame
    angle = phase.astype(jnp.float32) * (2.0 * math.pi / frame)
    scale = 1.0 / math.sqrt(frame)
    return (jnp.cos(angle) * scale, sign * jnp.sin(angle) * scale)


def transform(real_part, imag_part, table_re, table_im):
    left_re = jnp.einsum("jk,skl->sjl", table_re, real_part, precision=high) - jnp.einsum(
        "jk,skl->sjl", table_im, imag_part, precision=high
    )
    left_im = jnp.einsum("jk,skl->sjl", table_re, imag_part, precision=high) + jnp.einsum(
        "jk,skl->sjl", table_im, real_part, precision=high
    )
    out_re = jnp.einsum("sjk,kl->sjl", left_re, table_re, precision=high) - jnp.einsum(
        "sjk,kl->sjl", left_im, table_im, precision=high
    )
    out_im = jnp.einsum("sjk,kl->sjl", left_re, table_im, precision=high) + jnp.einsum(
        "sjk,kl->sjl", left_im, table_re, precision=high
    )
    return (out_re, out_im)


def per_device(obj_field, eigenprobes, weights, offsets, counts, amplitudes):
    tile = obj_field.shape[1]
    modes = eigenprobes.shape[1]
    frame = eigenprobes.shape[2]
    slots = weights.shape[2]
    n_tx = lax.axis_size("tx")
    n_chip = lax.axis_size("ty_0")
    n_core = lax.axis_size("ty_1")
    n_ty = n_chip * n_core
    share = frame // n_chip
    per_tx = modes // n_tx
    wts = weights[0, 0]
    offs = offsets[0, 0]
    live = (jnp.arange(slots, dtype=jnp.int32) < counts[0, 0]).astype(jnp.float32)
    live_wts = live[:, None] * wts
    below = moved(obj_field, -1, 0)
    beside = moved(obj_field, 0, -1)
    corner = moved(obj_field, -1, -1)
    region = jnp.concatenate(
        [
            jnp.concatenate([obj_field, beside], axis=2),
            jnp.concatenate([below, corner], axis=2),
        ],
        axis=1,
    )
    zero_index = jnp.int32(0)
    windows = jnp.stack(
        [
            lax.dynamic_slice(region, (zero_index, offs[s, 0], offs[s, 1]), (2, frame, frame))
            for s in range(slots)
        ]
    )
    win_re = windows[:, 0]
    win_im = windows[:, 1]
    eig32 = eigenprobes.astype(jnp.float32)
    probe = jnp.einsum("sk,ckij->csij", wts, eig32, precision=high)
    psi_re = probe[0] * win_re - probe[1] * win_im
    psi_im = probe[0] * win_im + probe[1] * win_re
    fwd_re, fwd_im = tables(frame, -1.0)
    spec_re, spec_im = transform(psi_re, psi_im, fwd_re, fwd_im)
    amps = amplitudes[0, 0].astype(jnp.float32)
    factor = (amps / jnp.sqrt(spec_re * spec_re + spec_im * spec_im + 0.25) - 1.0) * live[
        :, None, None
    ]
    inv_re, inv_im = tables(frame, 1.0)
    chi_re, chi_im = transform(spec_re * factor, spec_im * factor, inv_re, inv_im)
    grad_re = win_re * chi_re + win_im * chi_im
    grad_im = win_re * chi_im - win_im * chi_re
    power = (probe[0] * probe[0] + probe[1] * probe[1]) * live[:, None, None]
    local_illum = jnp.sum(power)

    grads = jnp.stack([grad_re, grad_im]).reshape(2, slots, n_chip, share, frame)
    grads = grads.transpose(2, 0, 1, 3, 4).reshape(n_ty, slots * share, frame)
    note = jnp.zeros((8, frame), jnp.float32)
    note = note.at[0, : slots * modes].set(live_wts.reshape(-1))
    note = note.at[1, :].set(local_illum)
    packed = jnp.concatenate([grads, jnp.broadcast_to(note[None], (n_ty, 8, frame))], axis=1)
    row = exchanged(packed, TY)
    row_wts = row[:, slots * share, : slots * modes].reshape(n_ty * slots, modes)
    row_grads = row[:, : slots * share].reshape(n_ty * slots, share, frame)
    row_illum = jnp.sum(row[:, slots * share + 1, 0])
    mode_grads = jnp.einsum("pk,pij->kij", row_wts, row_grads, precision=high)
    row_norms = jnp.sum(row_wts * row_wts, axis=0)
    tail = jnp.broadcast_to(row_norms[:, None, None], (modes, 4, frame))
    tail = jnp.concatenate([tail, jnp.full((modes, 4, frame), row_illum)], axis=1)
    sent = jnp.concatenate([mode_grads, tail], axis=1)
    total = exchanged(sent, "tx").reshape(n_tx, per_tx, share + 8, frame).sum(axis=0)
    illum_sum = total[0, share + 4, 0]
    start_mode = lax.axis_index("tx") * per_tx
    core = lax.axis_index("ty_1")
    own = lax.dynamic_slice(
        eigenprobes,
        (core, start_mode, lax.axis_index("ty_0") * share, zero_index),
        (1, per_tx, share, frame),
    )[0].astype(jnp.float32)
    updated = own + total[:, :share] / (total[:, share : share + 1] + 1.0)
    column = copied_to_all(updated, "tx").reshape(modes, share, frame)
    half = copied_to_all(column, "ty_0").reshape(n_chip, modes, share, frame)
    other = lax.ppermute(half, "ty_1", [(0, 1), (1, 0)])
    half = half.transpose(1, 0, 2, 3).reshape(modes, frame, frame)
    other = other.transpose(1, 0, 2, 3).reshape(modes, frame, frame)
    first = core == 0
    new_eig = jnp.stack([jnp.where(first, half, other), jnp.where(first, other, half)])

    obj_re = probe[0] * chi_re + probe[1] * chi_im
    obj_im = probe[0] * chi_im - probe[1] * chi_re
    pieces = jnp.stack([obj_re, obj_im, power], axis=1)
    acc = jnp.zeros((3, tile + frame, tile + frame), jnp.float32)
    for s in range(slots):
        at = (zero_index, offs[s, 0], offs[s, 1])
        current = lax.dynamic_slice(acc, at, (3, frame, frame))
        acc = lax.dynamic_update_slice(acc, current + pieces[s], at)
    from_left = moved(acc[:, :tile, tile:], 0, 1)
    from_above = moved(acc[:, tile:, :tile], 1, 0)
    from_corner = moved(acc[:, tile:, tile:], 1, 1)
    totals = acc[:, :tile, :tile] + from_left + from_above + from_corner
    cells = n_tx * n_ty * tile * tile
    mean_illum = illum_sum / cells
    new_object = obj_field + totals[:2] / (totals[2] + mean_illum)[None]
    return (new_object, new_eig)


def solution(mesh):
    finer = Mesh(
        mesh.devices.reshape(mesh.shape["grp"], mesh.shape["tx"], -1, 2),
        ("grp", "tx", "ty_0", "ty_1"),
    )
    return jax.shard_map(
        per_device,
        mesh=finer,
        in_specs=(
            P(None, ("grp", "tx"), TY),
            P(None, "grp", None, None),
            P(("grp", "tx"), TY, None, None),
            P(("grp", "tx"), TY, None, None),
            P(("grp", "tx"), TY),
            P(("grp", "tx"), TY, None, None, None),
        ),
        out_specs=(P(None, ("grp", "tx"), TY), P(None, "grp", None, None)),
        check_vma=False,
    )
```

```python
import functools
import math

import jax
import jax.numpy as jnp
import numpy as np
from jax import lax
from jax.experimental import pallas as pl
from jax.experimental.pallas import tpu as pltpu
from jax.sharding import Mesh
from jax.sharding import PartitionSpec as P

TY = ("ty_0", "ty_1")
PART = ("tx", "ty_0", "ty_1")

high = lax.Precision.HIGHEST
three = lax.Precision.HIGH

IN_VMEM = pl.BlockSpec(memory_space=pltpu.VMEM)
IN_SMEM = pl.BlockSpec(memory_space=pltpu.SMEM)


def moved(value, down, right):
    rows = lax.axis_size("tx")
    cols = lax.axis_size("ty_0") * lax.axis_size("ty_1")
    pairs = [
        (i * cols + j, ((i + down) % rows) * cols + (j + right) % cols)
        for i in range(rows)
        for j in range(cols)
    ]
    return lax.ppermute(value, PART, pairs)


def exchanged(blocks, axis):
    return lax.all_to_all(blocks, axis, split_axis=0, concat_axis=0, tiled=True)


def copied_to_all(block, axis):
    count = lax.axis_size(axis)
    return exchanged(jnp.broadcast_to(block[None], (count, *block.shape)), axis)


def tables(frame):
    grid = np.arange(frame)
    angle = (grid[:, None] * grid[None, :] % frame) * (2.0 * math.pi / frame)
    scale = 1.0 / math.sqrt(frame)
    return np.stack([np.cos(angle) * scale, np.sin(angle) * scale]).astype(np.float32)


def eights(start):
    base = pl.multiple_of((start // 8) * 8, 8)
    return base, start - base


def probe_kernel(wts, counts, eig, probe, note, *, slots, modes):
    frame = eig.shape[2]
    rows = 32
    count = counts[0, 0]
    sums = []
    for s in range(slots):
        sums.append(jnp.zeros((rows, frame), jnp.float32))
    for start in range(0, frame, rows):
        at = pl.ds(start, rows)
        parts = [[jnp.zeros((rows, frame), jnp.float32) for _ in range(slots)] for _ in range(2)]
        for k in range(modes):
            for c in range(2):
                image = eig[c, k, at, :].astype(jnp.float32)
                for s in range(slots):
                    parts[c][s] = parts[c][s] + wts[s, k] * image
        for s in range(slots):
            probe[0, s, at, :] = parts[0][s]
            probe[1, s, at, :] = parts[1][s]
            sums[s] = sums[s] + parts[0][s] * parts[0][s] + parts[1][s] * parts[1][s]
    total = jnp.zeros((rows, frame), jnp.float32)
    for s in range(slots):
        total = total + jnp.where(s < count, sums[s], 0.0)
    illum = jnp.sum(total)
    row = lax.broadcasted_iota(jnp.int32, (8, frame), 0)
    lane = lax.broadcasted_iota(jnp.int32, (8, frame), 1)
    lane = jnp.where(row == 0, lane, -1)
    value = jnp.where(row == 1, illum, 0.0)
    for s in range(slots):
        live = jnp.where(s < count, 1.0, 0.0)
        for k in range(modes):
            value = jnp.where(lane == s * modes + k, live * wts[s, k], value)
    note[...] = value


def frame_kernel(
    offs, counts, table, obj, beside, below, corner, probe, amps, note,
    grads, kept, right, down, across,
    region, acc, win, *, slots, share, n_core,
):
    frame = obj.shape[1]
    wide = 2 * frame
    count = counts[0, 0]
    for c in range(2):
        region[c, :frame, :frame] = obj[c]
        region[c, :frame, frame:] = beside[c]
        region[c, frame:, :frame] = below[c]
        region[c, frame:, frame:] = corner[c]
    acc[...] = jnp.zeros_like(acc)
    for s in range(slots):
        base, rest = eights(offs[s, 0])
        col = offs[s, 1]
        for c in range(2):
            tall = region[c, pl.ds(base, frame + 8), :]
            tall = pltpu.roll(tall, (frame + 8 - rest) % (frame + 8), 0)[:frame]
            win[c, s] = pltpu.roll(tall, (wide - col) % wide, 1)[:, :frame]
    cos = table[0]
    sin = table[1]
    stacked = jnp.concatenate([cos, sin], axis=0)
    side = jnp.concatenate([cos, sin], axis=1)

    def transform(reals, imags, sign):
        both = jnp.concatenate(reals + imags, axis=1)
        left = jnp.dot(stacked, both, precision=three, preferred_element_type=jnp.float32)
        up, low = left[:frame], left[frame:]
        half = slots * frame
        mid = []
        for s in range(slots):
            a = s * frame
            mid.append(up[:, a : a + frame] + sign * low[:, half + a : half + a + frame])
        for s in range(slots):
            a = s * frame
            mid.append(up[:, half + a : half + a + frame] - sign * low[:, a : a + frame])
        tall = jnp.concatenate(mid, axis=0)
        out = jnp.dot(tall, side, precision=three, preferred_element_type=jnp.float32)
        out_re, out_im = [], []
        for s in range(slots):
            a = s * frame
            re, im = out[a : a + frame], out[half + a : half + a + frame]
            out_re.append(re[:, :frame] + sign * im[:, frame:])
            out_im.append(im[:, :frame] - sign * re[:, frame:])
        return out_re, out_im

    psi_re, psi_im = [], []
    for s in range(slots):
        psi_re.append(probe[0, s] * win[0, s] - probe[1, s] * win[1, s])
        psi_im.append(probe[0, s] * win[1, s] + probe[1, s] * win[0, s])
    spec_re, spec_im = transform(psi_re, psi_im, 1.0)
    for s in range(slots):
        live = jnp.where(s < count, 1.0, 0.0)
        power = spec_re[s] * spec_re[s] + spec_im[s] * spec_im[s] + 0.25
        factor = (amps[s].astype(jnp.float32) / jnp.sqrt(power) - 1.0) * live
        spec_re[s] = spec_re[s] * factor
        spec_im[s] = spec_im[s] * factor
    chi_re, chi_im = transform(spec_re, spec_im, -1.0)
    for s in range(slots):
        live = jnp.where(s < count, 1.0, 0.0)
        image = (
            win[0, s] * chi_re[s] + win[1, s] * chi_im[s],
            win[0, s] * chi_im[s] - win[1, s] * chi_re[s],
        )
        for d in range(grads.shape[0]):
            a = (d // n_core) * share
            grads[d, s * share : (s + 1) * share, :] = image[d % n_core][a : a + share]
        pieces = (
            probe[0, s] * chi_re[s] + probe[1, s] * chi_im[s],
            probe[0, s] * chi_im[s] - probe[1, s] * chi_re[s],
            (probe[0, s] * probe[0, s] + probe[1, s] * probe[1, s]) * live,
        )
        base, rest = eights(offs[s, 0])
        col = offs[s, 1]
        at = pl.ds(base, frame + 8)
        for q in range(3):
            spread = jnp.concatenate([pieces[q], jnp.zeros_like(pieces[q])], axis=1)
            spread = pltpu.roll(spread, col, 1)
            spread = jnp.concatenate([spread, jnp.zeros((8, wide), jnp.float32)], axis=0)
            acc[q, at, :] = acc[q, at, :] + pltpu.roll(spread, rest, 0)
    for d in range(grads.shape[0]):
        grads[d, slots * share :, :] = note[...]
    for q in range(3):
        kept[q] = acc[q, :frame, :frame]
        right[q] = acc[q, :frame, frame:]
        down[q] = acc[q, frame:, :frame]
        across[q] = acc[q, frame:, frame:]


def mode_kernel(row, sent, *, slots, modes, share):
    sources, depth, frame = row.shape
    notes = jnp.concatenate([row[d, slots * share : slots * share + 1, :] for d in range(sources)], axis=0)
    wts = jnp.concatenate([notes[:, s * modes : (s + 1) * modes] for s in range(slots)], axis=0)
    columns = []
    for r in range(share):
        columns.append(
            jnp.concatenate(
                [
                    jnp.concatenate([row[d, s * share + r : s * share + r + 1, :] for d in range(sources)], axis=0)
                    for s in range(slots)
                ],
                axis=0,
            )
        )
    dims = (((0,), (0,)), ((), ()))
    images = lax.dot_general(
        wts, jnp.concatenate(columns, axis=1), dims, precision=high, preferred_element_type=jnp.float32
    )
    norms = lax.dot_general(
        wts * wts, jnp.ones((slots * sources, frame), jnp.float32), dims,
        precision=high, preferred_element_type=jnp.float32,
    )
    illum = jnp.zeros((1, frame), jnp.float32)
    for d in range(sources):
        illum = illum + row[d, slots * share + 1 : slots * share + 2, :]
    for r in range(share):
        sent[:, r, :] = images[:, r * frame : (r + 1) * frame]
    sent[:, share, :] = norms
    for r in range(share + 1, share + 8):
        sent[:, r, :] = jnp.broadcast_to(illum, (modes, frame))


def update_kernel(parts, own, copies, illum, *, share):
    total = parts[0]
    for d in range(1, parts.shape[0]):
        total = total + parts[d]
    fresh = own[...].astype(jnp.float32) + total[:share] / (total[share : share + 1] + 1.0)
    for d in range(copies.shape[0]):
        copies[d] = fresh
    illum[...] = total[share:]


def per_device(obj_field, eigenprobes, weights, offsets, counts, amplitudes):
    tile = obj_field.shape[1]
    modes = eigenprobes.shape[1]
    frame = eigenprobes.shape[2]
    slots = weights.shape[2]
    n_tx = lax.axis_size("tx")
    n_chip = lax.axis_size("ty_0")
    n_core = lax.axis_size("ty_1")
    n_ty = n_chip * n_core
    share = frame // n_chip
    f32 = jnp.float32
    wts = weights[0, 0]
    offs = offsets[0, 0]
    below = moved(obj_field, -1, 0)
    beside = moved(obj_field, 0, -1)
    corner = moved(obj_field, -1, -1)
    probe, note = pl.pallas_call(
        functools.partial(probe_kernel, slots=slots, modes=modes),
        out_shape=(
            jax.ShapeDtypeStruct((2, slots, frame, frame), f32),
            jax.ShapeDtypeStruct((8, frame), f32),
        ),
        in_specs=[IN_SMEM, IN_SMEM, IN_VMEM],
        out_specs=(IN_VMEM, IN_VMEM),
    )(wts, counts, eigenprobes)
    core = lax.axis_index("ty_1")
    own = lax.dynamic_slice(
        eigenprobes,
        (core, lax.axis_index("tx"), lax.axis_index("ty_0") * share, jnp.int32(0)),
        (1, 1, share, frame),
    )[0, 0]
    quadrant = jax.ShapeDtypeStruct((3, tile, tile), f32)
    grads, kept, right, down, across = pl.pallas_call(
        functools.partial(frame_kernel, slots=slots, share=share, n_core=n_core),
        out_shape=(
            jax.ShapeDtypeStruct((n_ty, slots * share + 8, frame), f32),
            quadrant, quadrant, quadrant, quadrant,
        ),
        in_specs=[IN_SMEM, IN_SMEM] + [IN_VMEM] * 8,
        out_specs=(IN_VMEM,) * 5,
        scratch_shapes=[
            pltpu.VMEM((2, 2 * frame, 2 * frame), f32),
            pltpu.VMEM((3, 2 * frame, 2 * frame), f32),
            pltpu.VMEM((2, slots, frame, frame), f32),
        ],
    )(offs, counts, tables(frame), obj_field, beside, below, corner, probe, amplitudes[0, 0], note)
    row = exchanged(grads, TY)
    from_left = moved(right, 0, 1)
    from_above = moved(down, 1, 0)
    from_corner = moved(across, 1, 1)
    sent = pl.pallas_call(
        functools.partial(mode_kernel, slots=slots, modes=modes, share=share),
        out_shape=jax.ShapeDtypeStruct((modes, share + 8, frame), f32),
        in_specs=[IN_VMEM],
        out_specs=IN_VMEM,
    )(row)
    parts = exchanged(sent, "tx")
    copies, illum = pl.pallas_call(
        functools.partial(update_kernel, share=share),
        out_shape=(
            jax.ShapeDtypeStruct((n_tx, share, frame), f32),
            jax.ShapeDtypeStruct((8, frame), f32),
        ),
        in_specs=[IN_VMEM, IN_VMEM],
        out_specs=(IN_VMEM, IN_VMEM),
    )(parts, own)
    column = exchanged(copies, "tx")
    half = copied_to_all(column, "ty_0").reshape(n_chip, modes, share, frame)
    other = lax.ppermute(half, "ty_1", [(0, 1), (1, 0)])
    half = half.transpose(1, 0, 2, 3).reshape(modes, frame, frame)
    other = other.transpose(1, 0, 2, 3).reshape(modes, frame, frame)
    first = core == 0
    new_eig = jnp.stack([jnp.where(first, half, other), jnp.where(first, other, half)])

    totals = kept + from_left + from_above + from_corner
    cells = n_tx * n_ty * tile * tile
    mean_illum = illum[1, 0] / cells
    new_object = obj_field + totals[:2] / (totals[2] + mean_illum)[None]
    return (new_object, new_eig)


def solution(mesh):
    finer = Mesh(
        mesh.devices.reshape(mesh.shape["grp"], mesh.shape["tx"], -1, 2),
        ("grp", "tx", "ty_0", "ty_1"),
    )
    return jax.shard_map(
        per_device,
        mesh=finer,
        in_specs=(
            P(None, ("grp", "tx"), TY),
            P(None, "grp", None, None),
            P(("grp", "tx"), TY, None, None),
            P(("grp", "tx"), TY, None, None),
            P(("grp", "tx"), TY),
            P(("grp", "tx"), TY, None, None, None),
        ),
        out_specs=(P(None, ("grp", "tx"), TY), P(None, "grp", None, None)),
        check_vma=False,
    )
```
